32 devices in a mesh: real: 2 (over y), col: 8 (over z, x), row: 2 (over core).
Axes of the slice: x: 2, y: 2, z: 4, core: 2. Of those that a mesh axis runs over, the one named last changes fastest.
Arguments:
- theta: bfloat16 [512, 16384], P(('real', 'row'), 'col'), parts along dimension 0, may hold values from -6 to 6
- signs: int32 [32768], P(('real', 'col')), parts along dimension 0, may hold values from -1 to 1, as said below
- kept: int32 [1024], replicated, may hold values from 0 to 16383, as said below
Outputs:
- gram: float32 [4, 8, 16, 256], P(('real', 'row'), 'col'), parts along dimension 0
The draws below stay inside these ranges and needn't reach their ends.
There are 2 independent parts, one for each index of `real`. The reference program is written for one: setup_inputs(seed, part) draws one part's arguments, and reference() takes and returns one part's arrays. A program takes and returns all parts, laid end to end along the dimension named above; an argument that names none is the same for every part. Nothing has to cross between parts.
Inputs may be any that keep to these rules, and one draw needn't show every extreme that they name: `signs`: each entry is -1 or 1. `kept`: 1024 distinct column indices.
All inputs are finite; a program needn't handle non-finite values.
Results may differ from the reference program's by a relative error of at most 0.0036.
Values may be sent and summed in bfloat16 or wider, within the bound.
No kernel may reach another device: no remote copies, remote signals or barrier semaphores. Data moves between devices by JAX's collectives and lax.ppermute only.
A program may use at most 64 MiB of HBM per device.

```python
import jax
import jax.numpy as jnp
from jax import lax

SIDE = 128
N = 16384
KEEP = 1024
ROW_DEV = 16
ROWS = 256
N_COL = 8
N_ROW = 2


def draw_signs(key, part):
    return (2 * jax.random.randint(jax.random.fold_in(key, 11), (N,), 0, 2) - 1).astype(jnp.int32)


def draw_kept(key, part):
    middle = 1 + jax.random.permutation(jax.random.fold_in(key, 23), N - 2)[:KEEP - 2]
    ends = jnp.array([0, N - 1], dtype=jnp.int32)
    whole = jnp.concatenate([ends, middle.astype(jnp.int32)])
    order = jax.random.permutation(jax.random.fold_in(key, 29), KEEP)
    return whole[order].astype(jnp.int32)


def level_of(own_key, extent, cuts, low, top_value):
    loudness = 1.0
    for dim, parts in cuts:
        heights = jax.random.uniform(jax.random.fold_in(jax.random.fold_in(own_key, 6), dim), (parts,), jnp.float32, low / len(cuts), top_value / len(cuts))
        loudness = loudness * jnp.repeat(jnp.exp(heights), extent[dim] // parts).reshape((-1,) + (1,) * (len(extent) - 1 - dim))
    return loudness


def bell_draw(own_key, extent, spread, reach, cuts=(), kind=jnp.bfloat16):
    gain = level_of(own_key, extent, cuts, -0.22, 0.18) if cuts else 1.0
    values = jax.random.normal(own_key, extent, jnp.float32) * spread * gain
    return jnp.minimum(jnp.maximum(values, -reach), reach).astype(kind)


def setup_inputs(seed: int = 0, part: int = 0) -> dict:
    arg_keys = jax.random.split(jax.random.key(seed), 4)
    part_keys = jax.random.split(jax.random.fold_in(arg_keys[3], part), 4)
    theta = bell_draw(part_keys[0], (ROWS, N), 1.0, 6.0, ((0, 2), (1, 8)))
    signs = draw_signs(jax.random.fold_in(jax.random.fold_in(arg_keys[3], part), 71), part)
    kept = draw_kept(jax.random.fold_in(arg_keys[3], 71), part)
    return {"theta": theta, "signs": signs, "kept": kept}


def hadamard(order, dtype):
    indices = jnp.arange(order, dtype=jnp.int32)
    common = indices[:, None] & indices[None, :]
    parity = jnp.zeros((order, order), jnp.int32)
    for position in range(order.bit_length() - 1):
        parity = parity ^ ((common >> position) & 1)
    return (1 - 2 * parity).astype(dtype)


def reference(theta, signs, kept):
    scaled = theta * signs.astype(jnp.bfloat16)[None, :]
    flat = scaled.astype(jnp.float32).reshape(ROWS * SIDE, SIDE)
    table = hadamard(SIDE, jnp.float32)
    inner = jnp.dot(flat, table, precision=lax.Precision.HIGHEST).reshape(ROWS, SIDE, SIDE)
    outer = jnp.einsum("rak,aj->rjk", inner, table, precision=lax.Precision.HIGHEST)
    transformed = outer.reshape(ROWS, N) / SIDE
    sketch = jnp.take(transformed, kept.astype(jnp.int32), axis=1).astype(jnp.bfloat16)
    widened = sketch.astype(jnp.float32)
    gram = jnp.dot(widened, widened.T, precision=lax.Precision.HIGHEST) / KEEP
    return gram.reshape(N_ROW, N_COL, ROW_DEV, ROWS)
```

```python
import functools

import jax
import jax.numpy as jnp
from jax import lax
from jax.experimental import pallas as pl
from jax.experimental.pallas import tpu as pltpu
from jax.sharding import PartitionSpec as P

SIDE = 128


def sign_of(bits, shift=4):
    while shift:
        bits = bits ^ bits >> shift
        shift //= 2
    return (1 - 2 * (bits & 1)).astype(jnp.float32).astype(jnp.bfloat16)


def partial_kernel(theta_ref, signs_ref, kept_ref, out_ref, table_ref, *, by_block):
    rows, local = theta_ref.shape
    keep = kept_ref.shape[1]
    groups = local // SIDE
    first = lax.axis_index("col") * groups
    kept = kept_ref[...]
    low = sign_of(lax.broadcasted_iota(jnp.int32, (SIDE, keep), 0) & kept)
    for group in range(groups):
        high = sign_of((kept >> 7) & (first + group))
        table_ref[group * SIDE : (group + 1) * SIDE, :] = low * high
    scaled = theta_ref[...] * signs_ref[...].astype(jnp.float32).astype(jnp.bfloat16)
    part = jnp.dot(scaled, table_ref[...], preferred_element_type=jnp.float32)
    if by_block:
        width = out_ref.shape[2]
        for block in range(out_ref.shape[0]):
            out_ref[block] = part[:, block * width : (block + 1) * width].astype(jnp.bfloat16)
    else:
        out_ref[...] = part.T.astype(jnp.bfloat16)


def partial_sketch(theta, signs, kept, parts):
    rows, local = theta.shape
    keep = kept.shape[0]
    width = keep // parts
    by_block = width % SIDE == 0
    shape = (parts, rows, width) if by_block else (keep, rows)
    out = pl.pallas_call(
        functools.partial(partial_kernel, by_block=by_block),
        out_shape=jax.ShapeDtypeStruct(shape, jnp.bfloat16),
        in_specs=[pl.BlockSpec(memory_space=pltpu.VMEM)] * 3,
        out_specs=pl.BlockSpec(memory_space=pltpu.VMEM),
        scratch_shapes=[pltpu.VMEM((local, keep), jnp.bfloat16)],
        name="partial_sketch",
    )(theta, signs.reshape(1, local), kept.reshape(1, keep))
    return out if by_block else out.reshape(parts, width, rows).swapaxes(1, 2)


def per_device(parts, halves, length, theta, signs, kept):
    keep = kept.shape[0]
    rows = theta.shape[0]
    part = partial_sketch(theta, signs, kept, parts)
    met = lax.all_to_all(part, "col", split_axis=0, concat_axis=0, tiled=True)
    sketch = (met.astype(jnp.float32).sum(0) / SIDE).astype(jnp.bfloat16)
    other = lax.ppermute(sketch, "row", [(i, (i + 1) % halves) for i in range(halves)])
    own = lax.axis_index("row") == 0
    both = jnp.concatenate([jnp.where(own, sketch, other), jnp.where(own, other, sketch)], axis=0)
    gram = jnp.dot(sketch, both.T, preferred_element_type=jnp.float32).astype(jnp.bfloat16)
    met = lax.all_to_all(gram.reshape(parts, rows // parts, -1), "col", split_axis=0, concat_axis=0, tiled=True)
    return (met.astype(jnp.float32).sum(0) / keep)[None, None]


def solution(mesh):
    parts, halves = mesh.shape["col"], mesh.shape["row"]
    return jax.shard_map(
        functools.partial(per_device, parts, halves, None),
        mesh=mesh,
        in_specs=(P(("real", "row"), "col"), P(("real", "col")), P()),
        out_specs=P(("real", "row"), "col", None, None),
        check_vma=False,
    )
```

```python
import functools

import jax
import jax.numpy as jnp
from jax import lax
from jax.experimental import pallas as pl
from jax.experimental.pallas import tpu as pltpu
from jax.sharding import PartitionSpec as P

SIDE = 128
STRIPS = 4


def sign_of(bits, shift=4):
    while shift:
        bits = bits ^ bits >> shift
        shift //= 2
    return (1 - 2 * (bits & 1)).astype(jnp.float32).astype(jnp.bfloat16)


def partial_kernel(theta_hbm, signs_hbm, kept_hbm, out_ref, theta_ref, signs_ref, kept_ref, table_ref, sems, *, by_block):
    copies = [
        pltpu.make_async_copy(source, target, sems.at[i])
        for i, (source, target) in enumerate(((kept_hbm, kept_ref), (signs_hbm, signs_ref), (theta_hbm, theta_ref)))
    ]
    for copy in copies:
        copy.start()
    rows, local = theta_ref.shape
    keep = kept_ref.shape[1]
    groups = local // SIDE
    first = lax.axis_index("col") * groups
    strip = keep // STRIPS

    def build(s):
        kept = kept_ref[:, s * strip : (s + 1) * strip]
        low = sign_of(lax.broadcasted_iota(jnp.int32, (SIDE, strip), 0) & kept)
        high = sign_of((first + lax.broadcasted_iota(jnp.int32, (groups, strip), 0)) & (kept >> 7))
        for group in range(groups):
            table_ref[group * SIDE : (group + 1) * SIDE, s * strip : (s + 1) * strip] = low * high[group : group + 1]

    copies[0].wait()
    build(0)
    copies[1].wait()
    copies[2].wait()
    theta_ref[...] = theta_ref[...] * signs_ref[...].astype(jnp.float32).astype(jnp.bfloat16)
    for s in range(STRIPS):
        if s + 1 < STRIPS:
            build(s + 1)
        part = jnp.dot(theta_ref[...], table_ref[:, s * strip : (s + 1) * strip], preferred_element_type=jnp.float32)
        if by_block:
            width = out_ref.shape[2]
            for block in range(strip // width):
                out_ref[s * (strip // width) + block] = part[:, block * width : (block + 1) * width].astype(jnp.bfloat16)
        else:
            out_ref[s * strip : (s + 1) * strip, :] = part.T.astype(jnp.bfloat16)


def partial_sketch(theta, signs, kept, parts):
    rows, local = theta.shape
    keep = kept.shape[0]
    width = keep // parts
    by_block = width % SIDE == 0
    shape = (parts, rows, width) if by_block else (keep, rows)
    inputs = (theta, signs.reshape(1, local), kept.reshape(1, keep))
    out = pl.pallas_call(
        functools.partial(partial_kernel, by_block=by_block),
        out_shape=pltpu.VMEM(shape, jnp.bfloat16),
        in_specs=[pl.BlockSpec(memory_space=pltpu.HBM)] * 3,
        out_specs=pl.BlockSpec(memory_space=pltpu.VMEM),
        scratch_shapes=[
            pltpu.VMEM((rows, local), jnp.bfloat16),
            pltpu.VMEM((1, local), jnp.int32),
            pltpu.VMEM((1, keep), jnp.int32),
            pltpu.VMEM((local, keep), jnp.bfloat16),
            pltpu.SemaphoreType.DMA((3,)),
        ],
        compiler_params=pltpu.CompilerParams(vmem_limit_bytes=32 << 20),
        name="partial_sketch",
    )(*(pltpu.with_memory_space_constraint(x, pltpu.HBM) for x in inputs))
    return out if by_block else out.reshape(parts, width, rows).swapaxes(1, 2)


def per_device(parts, halves, theta, signs, kept):
    keep = kept.shape[0]
    rows = theta.shape[0]
    part = partial_sketch(theta, signs, kept, parts)
    met = lax.all_to_all(part, "col", split_axis=0, concat_axis=0, tiled=True)
    sketch = (met.astype(jnp.float32).sum(0) / SIDE).astype(jnp.bfloat16)
    other = lax.ppermute(sketch, "row", [(i, (i + 1) % halves) for i in range(halves)])
    own = lax.axis_index("row") == 0
    both = jnp.concatenate([jnp.where(own, sketch, other), jnp.where(own, other, sketch)], axis=0)
    gram = jnp.dot(sketch, both.T, preferred_element_type=jnp.float32).astype(jnp.bfloat16)
    met = lax.all_to_all(gram.reshape(parts, rows // parts, -1), "col", split_axis=0, concat_axis=0, tiled=True)
    return (met.astype(jnp.float32).sum(0) / keep)[None, None]


def solution(mesh):
    return jax.shard_map(
        functools.partial(per_device, mesh.shape["col"], mesh.shape["row"]),
        mesh=mesh,
        in_specs=(P(("real", "row"), "col"), P(("real", "col")), P()),
        out_specs=P(("real", "row"), "col", None, None),
        check_vma=False,
    )
```

```python
import functools

import jax
import jax.numpy as jnp
from jax import lax
from jax.experimental import pallas as pl
from jax.experimental.pallas import tpu as pltpu
from jax.sharding import PartitionSpec as P

SIDE = 128
STRIPS = 4


def sign_of(bits, shift=4):
    while shift:
        bits = bits ^ bits >> shift
        shift //= 2
    return (1 - 2 * (bits & 1)).astype(jnp.float32).astype(jnp.bfloat16)


def partial_kernel(theta_hbm, signs_hbm, kept_hbm, out_ref, row_ref, theta_ref, signs_ref, kept_ref, table_ref, sems, *, by_block):
    copies = [
        pltpu.make_async_copy(source, target, sems.at[i])
        for i, (source, target) in enumerate(((kept_hbm, kept_ref), (signs_hbm, signs_ref), (theta_hbm, theta_ref)))
    ]
    for copy in copies:
        copy.start()
    rows, local = theta_ref.shape
    keep = kept_ref.shape[1]
    groups = local // SIDE
    first = lax.axis_index("col") * groups
    strip = keep // STRIPS

    def build(s):
        kept = kept_ref[:, s * strip : (s + 1) * strip]
        low = sign_of(lax.broadcasted_iota(jnp.int32, (SIDE, strip), 0) & kept)
        high = sign_of((first + lax.broadcasted_iota(jnp.int32, (groups, strip), 0)) & (kept >> 7))
        for group in range(groups):
            table_ref[group * SIDE : (group + 1) * SIDE, s * strip : (s + 1) * strip] = low * high[group : group + 1]

    row_ref[...] = jnp.full(row_ref.shape, lax.axis_index("row"), jnp.int32)
    copies[0].wait()
    build(0)
    copies[1].wait()
    copies[2].wait()
    theta_ref[...] = theta_ref[...] * signs_ref[...].astype(jnp.float32).astype(jnp.bfloat16)
    for s in range(STRIPS):
        if s + 1 < STRIPS:
            build(s + 1)
        part = jnp.dot(theta_ref[...], table_ref[:, s * strip : (s + 1) * strip], preferred_element_type=jnp.float32)
        if by_block:
            width = out_ref.shape[2]
            for block in range(strip // width):
                out_ref[s * (strip // width) + block] = part[:, block * width : (block + 1) * width].astype(jnp.bfloat16)
        else:
            out_ref[s * strip : (s + 1) * strip, :] = part.T.astype(jnp.bfloat16)


def partial_sketch(theta, signs, kept, parts):
    rows, local = theta.shape
    keep = kept.shape[0]
    width = keep // parts
    by_block = width % SIDE == 0
    shape = (parts, rows, width) if by_block else (keep, rows)
    inputs = (theta, signs.reshape(1, local), kept.reshape(1, keep))
    out, row = pl.pallas_call(
        functools.partial(partial_kernel, by_block=by_block),
        out_shape=(pltpu.VMEM(shape, jnp.bfloat16), pltpu.VMEM((1, width), jnp.int32)),
        in_specs=[pl.BlockSpec(memory_space=pltpu.HBM)] * 3,
        out_specs=(pl.BlockSpec(memory_space=pltpu.VMEM),) * 2,
        scratch_shapes=[
            pltpu.VMEM((rows, local), jnp.bfloat16),
            pltpu.VMEM((1, local), jnp.int32),
            pltpu.VMEM((1, keep), jnp.int32),
            pltpu.VMEM((local, keep), jnp.bfloat16),
            pltpu.SemaphoreType.DMA((3,)),
        ],
        compiler_params=pltpu.CompilerParams(vmem_limit_bytes=32 << 20),
        name="partial_sketch",
    )(*(pltpu.with_memory_space_constraint(x, pltpu.HBM) for x in inputs))
    return (out if by_block else out.reshape(parts, width, rows).swapaxes(1, 2)), row


def exchange(blocks, order):
    return lax.all_to_all(blocks, "col", split_axis=0, concat_axis=0, tiled=True, axis_index_groups=[order])


def per_device(parts, halves, theta, signs, kept):
    keep = kept.shape[0]
    rows = theta.shape[0]
    order = [(parts // 2 - i) % parts for i in range(parts)]
    part, row = partial_sketch(theta, signs, kept, parts)
    met, row = lax.optimization_barrier((exchange(part, order), row))
    sketch = (met.astype(jnp.float32).sum(0) / SIDE).astype(jnp.bfloat16)
    other = lax.ppermute(sketch, "row", [(i, (i + 1) % halves) for i in range(halves)])
    own = row == 0
    both = jnp.concatenate([jnp.where(own, sketch, other), jnp.where(own, other, sketch)], axis=0)
    blocks = sketch.reshape(parts, rows // parts, -1)
    ordered = jnp.concatenate([blocks[i] for i in order], axis=0)
    gram = jnp.dot(ordered, both.T, preferred_element_type=jnp.float32).astype(jnp.bfloat16)
    met = exchange(gram.reshape(parts, rows // parts, -1), order)
    return (met.astype(jnp.float32).sum(0) / keep)[None, None]


def solution(mesh):
    return jax.shard_map(
        functools.partial(per_device, mesh.shape["col"], mesh.shape["row"]),
        mesh=mesh,
        in_specs=(P(("real", "row"), "col"), P(("real", "col")), P()),
        out_specs=P(("real", "row"), "col", None, None),
        check_vma=False,
    )
```

```python
import functools

import jax
import jax.numpy as jnp
from jax import lax
from jax.experimental import pallas as pl
from jax.experimental.pallas import tpu as pltpu
from jax.sharding import PartitionSpec as P

SIDE = 128
STRIPS = 4


def sign_of(bits, shift=4):
    while shift:
        bits = bits ^ bits >> shift
        shift //= 2
    return (1 - 2 * (bits & 1)).astype(jnp.float32).astype(jnp.bfloat16)


def partial_kernel(theta_hbm, signs_hbm, kept_hbm, out_ref, row_ref, theta_ref, signs_ref, kept_ref, table_ref, sems, *, by_block):
    copies = [
        pltpu.make_async_copy(source, target, sems.at[i])
        for i, (source, target) in enumerate(((kept_hbm, kept_ref), (signs_hbm, signs_ref), (theta_hbm, theta_ref)))
    ]
    for copy in copies:
        copy.start()
    rows, local = theta_ref.shape
    keep = kept_ref.shape[1]
    groups = local // SIDE
    first = lax.axis_index("col") * groups
    strip = keep // STRIPS

    def build(s):
        kept = kept_ref[:, s * strip : (s + 1) * strip]
        low = sign_of(lax.broadcasted_iota(jnp.int32, (SIDE, strip), 0) & kept)
        high = sign_of((first + lax.broadcasted_iota(jnp.int32, (groups, strip), 0)) & (kept >> 7))
        for group in range(groups):
            table_ref[group * SIDE : (group + 1) * SIDE, s * strip : (s + 1) * strip] = low * high[group : group + 1]

    row_ref[...] = jnp.full(row_ref.shape, lax.axis_index("row"), jnp.int32)
    copies[0].wait()
    build(0)
    copies[1].wait()
    copies[2].wait()
    theta_ref[...] = theta_ref[...] * signs_ref[...].astype(jnp.float32).astype(jnp.bfloat16)
    for s in range(STRIPS):
        if s + 1 < STRIPS:
            build(s + 1)
        part = jnp.dot(theta_ref[...], table_ref[:, s * strip : (s + 1) * strip], preferred_element_type=jnp.float32)
        if by_block:
            width = out_ref.shape[2]
            for block in range(strip // width):
                out_ref[s * (strip // width) + block] = part[:, block * width : (block + 1) * width].astype(jnp.bfloat16)
        else:
            out_ref[s * strip : (s + 1) * strip, :] = part.T.astype(jnp.bfloat16)


def partial_sketch(theta, signs, kept, parts):
    rows, local = theta.shape
    keep = kept.shape[0]
    width = keep // parts
    by_block = width % SIDE == 0
    shape = (parts, rows, width) if by_block else (keep, rows)
    inputs = (theta, signs.reshape(1, local), kept.reshape(1, keep))
    out, row = pl.pallas_call(
        functools.partial(partial_kernel, by_block=by_block),
        out_shape=(pltpu.VMEM(shape, jnp.bfloat16), pltpu.VMEM((1, width), jnp.int32)),
        in_specs=[pl.BlockSpec(memory_space=pltpu.HBM)] * 3,
        out_specs=(pl.BlockSpec(memory_space=pltpu.VMEM),) * 2,
        scratch_shapes=[
            pltpu.VMEM((rows, local), jnp.bfloat16),
            pltpu.VMEM((1, local), jnp.int32),
            pltpu.VMEM((1, keep), jnp.int32),
            pltpu.VMEM((local, keep), jnp.bfloat16),
            pltpu.SemaphoreType.DMA((3,)),
        ],
        compiler_params=pltpu.CompilerParams(vmem_limit_bytes=32 << 20),
        name="partial_sketch",
    )(*(pltpu.with_memory_space_constraint(x, pltpu.HBM) for x in inputs))
    return (out if by_block else out.reshape(parts, width, rows).swapaxes(1, 2)), row


def exchange(blocks, order):
    return lax.all_to_all(blocks, "col", split_axis=0, concat_axis=0, tiled=True, axis_index_groups=[order])


def per_device(parts, halves, theta, signs, kept):
    keep = kept.shape[0]
    rows = theta.shape[0]
    order = [(parts // 2 + 1 + 3 * i) % parts for i in range(parts)]
    part, row = partial_sketch(theta, signs, kept, parts)
    met, row = lax.optimization_barrier((exchange(part, order), row))
    sketch = (met.astype(jnp.float32).sum(0) / SIDE).astype(jnp.bfloat16)
    other = lax.ppermute(sketch, "row", [(i, (i + 1) % halves) for i in range(halves)])
    own = row == 0
    both = jnp.concatenate([jnp.where(own, sketch, other), jnp.where(own, other, sketch)], axis=0)
    blocks = sketch.reshape(parts, rows // parts, -1)
    ordered = jnp.concatenate([blocks[i] for i in order], axis=0)
    gram = jnp.dot(ordered, both.T, preferred_element_type=jnp.float32).astype(jnp.bfloat16)
    met = exchange(gram.reshape(parts, rows // parts, -1), order)
    return (met.astype(jnp.float32).sum(0) / keep)[None, None]


def solution(mesh):
    return jax.shard_map(
        functools.partial(per_device, mesh.shape["col"], mesh.shape["row"]),
        mesh=mesh,
        in_specs=(P(("real", "row"), "col"), P(("real", "col")), P()),
        out_specs=P(("real", "row"), "col", None, None),
        check_vma=False,
    )
```

```python
import functools

import jax
import jax.numpy as jnp
from jax import lax
from jax.experimental import pallas as pl
from jax.experimental.pallas import tpu as pltpu
from jax.sharding import PartitionSpec as P

SIDE = 128
STRIPS = 4
TILE = 16


def sign_of(bits, shift=4):
    while shift:
        bits = bits ^ bits >> shift
        shift //= 2
    return (1 - 2 * (bits & 1)).astype(jnp.float32).astype(jnp.bfloat16)


def partial_kernel(theta_hbm, signs_hbm, kept_hbm, out_ref, theta_ref, signs_ref, kept_ref, table_ref, sems):
    copies = [
        pltpu.make_async_copy(source, target, sems.at[i])
        for i, (source, target) in enumerate(((theta_hbm, theta_ref), (kept_hbm, kept_ref), (signs_hbm, signs_ref)))
    ]
    for copy in copies:
        copy.start()
    local = theta_ref.shape[1]
    keep = kept_ref.shape[1]
    groups = local // SIDE
    first = lax.axis_index("col") * groups
    strip = keep // STRIPS

    def sign_rows(count, bits):
        return sign_of(lax.broadcasted_iota(jnp.int32, (count, strip), 0) & bits)

    def build(s):
        kept = kept_ref[:, s * strip : (s + 1) * strip]
        low, middle = sign_rows(TILE, kept & (TILE - 1)), sign_rows(SIDE // TILE, kept // TILE & (SIDE // TILE - 1))
        inner = jnp.concatenate([low * middle[i : i + 1] for i in range(SIDE // TILE)], axis=0)
        high = sign_of((first + lax.broadcasted_iota(jnp.int32, (groups, strip), 0)) & (kept >> 7))
        for group in range(groups):
            table_ref[group * SIDE : (group + 1) * SIDE, s * strip : (s + 1) * strip] = inner * high[group : group + 1]

    copies[1].wait()
    build(0)
    build(1)
    copies[2].wait()
    copies[0].wait()
    theta_ref[...] = theta_ref[...] * signs_ref[...].astype(jnp.float32).astype(jnp.bfloat16)
    for s in range(STRIPS):
        if s + 2 < STRIPS:
            build(s + 2)
        part = jnp.dot(theta_ref[...], table_ref[:, s * strip : (s + 1) * strip], preferred_element_type=jnp.float32)
        out_ref[s * strip : (s + 1) * strip, :] = part.T.astype(jnp.bfloat16)


def partial_sketch(theta, signs, kept):
    rows, local = theta.shape
    keep = kept.shape[0]
    inputs = (theta, signs.reshape(1, local), kept.reshape(1, keep))
    return pl.pallas_call(
        partial_kernel,
        out_shape=pltpu.VMEM((keep, rows), jnp.bfloat16),
        in_specs=[pl.BlockSpec(memory_space=pltpu.HBM)] * 3,
        out_specs=pl.BlockSpec(memory_space=pltpu.VMEM),
        scratch_shapes=[
            pltpu.VMEM((rows, local), jnp.bfloat16),
            pltpu.VMEM((1, local), jnp.int32),
            pltpu.VMEM((1, keep), jnp.int32),
            pltpu.VMEM((local, keep), jnp.bfloat16),
            pltpu.SemaphoreType.DMA((3,)),
        ],
        compiler_params=pltpu.CompilerParams(vmem_limit_bytes=32 << 20),
        name="partial_sketch",
    )(*(pltpu.with_memory_space_constraint(x, pltpu.HBM) for x in inputs))


def gram_kernel(met_ref, out_ref, *, rows_of, targets, halves):
    sums = [
        sum(met_ref[i].astype(jnp.float32) for i, row in enumerate(rows_of) if row == half) * (1 / SIDE)
        for half in range(halves)
    ]
    columns = jnp.concatenate([total.astype(jnp.bfloat16) for total in sums], axis=1)
    grams = [
        jnp.dot(total.T.astype(jnp.bfloat16), columns, preferred_element_type=jnp.float32).astype(jnp.bfloat16)
        for total in sums
    ]
    block = out_ref.shape[1]
    for i, (col, row) in enumerate(targets):
        out_ref[i] = grams[row][col * block : (col + 1) * block]


def partial_gram(met, rows_of, targets, parts, rows, halves):
    return pl.pallas_call(
        functools.partial(gram_kernel, rows_of=rows_of, targets=targets, halves=halves),
        out_shape=pltpu.VMEM((len(targets), rows // parts, halves * rows), jnp.bfloat16),
        in_specs=[pl.BlockSpec(memory_space=pltpu.VMEM)],
        out_specs=pl.BlockSpec(memory_space=pltpu.VMEM),
        compiler_params=pltpu.CompilerParams(vmem_limit_bytes=16 << 20),
        name="partial_gram",
    )(met)


def exchange(blocks, axes, order):
    return lax.all_to_all(blocks, axes, split_axis=0, concat_axis=0, tiled=True, axis_index_groups=[order])


def by_pair(part, parts, halves):
    rows = part.shape[1]
    size = parts * halves
    leader = (parts // 2 + 2) * halves - 1
    first, second = ([(leader + step * i) % size for i in range(size)] for step in (7, 5))
    met = exchange(part.reshape(size, -1, rows), ("col", "row"), first)
    rows_of = [i % halves for i in first]
    targets = [(i // halves, i % halves) for i in second]
    return exchange(partial_gram(met, rows_of, targets, parts, rows, halves), ("col", "row"), second)


def by_column(part, parts, halves):
    rows = part.shape[1]
    order = [(parts // 2 + 1 + 3 * i) % parts for i in range(parts)]
    met = exchange(part.reshape(parts, -1, rows), "col", order)
    sketch = (met.astype(jnp.float32).sum(0) / SIDE).astype(jnp.bfloat16)
    both = lax.all_gather(sketch, "row", axis=1, tiled=True)
    gram = lax.dot_general(sketch, both, (((0,), (0,)), ((), ())), preferred_element_type=jnp.float32)
    blocks = gram.astype(jnp.bfloat16).reshape(parts, rows // parts, -1)
    return exchange(jnp.concatenate([blocks[i : i + 1] for i in order]), "col", order)


def per_device(parts, halves, theta, signs, kept):
    keep = kept.shape[0]
    part = partial_sketch(theta, signs, kept)
    whole_tiles = keep % (parts * halves * TILE) == 0
    met = (by_pair if whole_tiles else by_column)(part, parts, halves)
    return (met.astype(jnp.float32).sum(0) / keep)[None, None]


def solution(mesh):
    return jax.shard_map(
        functools.partial(per_device, mesh.shape["col"], mesh.shape["row"]),
        mesh=mesh,
        in_specs=(P(("real", "row"), "col"), P(("real", "col")), P()),
        out_specs=P(("real", "row"), "col", None, None),
        check_vma=False,
    )
```

```python
import functools

import jax
import jax.numpy as jnp
from jax import lax
from jax.experimental import pallas as pl
from jax.experimental.pallas import tpu as pltpu
from jax.sharding import PartitionSpec as P

SIDE = 128
STRIPS = 4
TILE = 16


def sign_of(bits, shift=4):
    while shift:
        bits = bits ^ bits >> shift
        shift //= 2
    return (1 - 2 * (bits & 1)).astype(jnp.float32).astype(jnp.bfloat16)


def partial_kernel(theta_hbm, signs_hbm, kept_hbm, out_ref, theta_ref, signs_ref, kept_ref, table_ref, sems):
    copies = [
        pltpu.make_async_copy(source, target, sems.at[i])
        for i, (source, target) in enumerate(((theta_hbm, theta_ref), (kept_hbm, kept_ref), (signs_hbm, signs_ref)))
    ]
    for copy in copies:
        copy.start()
    local = theta_ref.shape[1]
    keep = kept_ref.shape[1]
    groups = local // SIDE
    first = lax.axis_index("col") * groups
    strip = keep // STRIPS

    def sign_rows(count, bits):
        return sign_of(lax.broadcasted_iota(jnp.int32, (count, strip), 0) & bits)

    def build(s):
        kept = kept_ref[:, s * strip : (s + 1) * strip]
        low, middle = sign_rows(TILE, kept & (TILE - 1)), sign_rows(SIDE // TILE, kept // TILE & (SIDE // TILE - 1))
        inner = jnp.concatenate([low * middle[i : i + 1] for i in range(SIDE // TILE)], axis=0)
        high = sign_of((first + lax.broadcasted_iota(jnp.int32, (groups, strip), 0)) & (kept >> 7))
        for group in range(groups):
            table_ref[group * SIDE : (group + 1) * SIDE, s * strip : (s + 1) * strip] = inner * high[group : group + 1]

    copies[1].wait()
    build(0)
    build(1)
    copies[2].wait()
    copies[0].wait()
    theta_ref[...] = theta_ref[...] * signs_ref[...].astype(jnp.float32).astype(jnp.bfloat16)
    for s in range(STRIPS):
        if s + 2 < STRIPS:
            build(s + 2)
        part = jnp.dot(theta_ref[...], table_ref[:, s * strip : (s + 1) * strip], preferred_element_type=jnp.float32)
        out_ref[s * strip : (s + 1) * strip, :] = part.T.astype(jnp.bfloat16)


def partial_sketch(theta, signs, kept):
    rows, local = theta.shape
    keep = kept.shape[0]
    inputs = (theta, signs.reshape(1, local), kept.reshape(1, keep))
    return pl.pallas_call(
        partial_kernel,
        out_shape=pltpu.VMEM((keep, rows), jnp.bfloat16),
        in_specs=[pl.BlockSpec(memory_space=pltpu.HBM)] * 3,
        out_specs=pl.BlockSpec(memory_space=pltpu.VMEM),
        scratch_shapes=[
            pltpu.VMEM((rows, local), jnp.bfloat16),
            pltpu.VMEM((1, local), jnp.int32),
            pltpu.VMEM((1, keep), jnp.int32),
            pltpu.VMEM((local, keep), jnp.bfloat16),
            pltpu.SemaphoreType.DMA((3,)),
        ],
        compiler_params=pltpu.CompilerParams(vmem_limit_bytes=32 << 20),
        name="partial_sketch",
    )(*(pltpu.with_memory_space_constraint(x, pltpu.HBM) for x in inputs))


def gram_kernel(met_ref, out_ref, *, rows_of, targets, halves):
    sums = [
        sum(met_ref[i].astype(jnp.float32) for i, row in enumerate(rows_of) if row == half) * (1 / SIDE)
        for half in range(halves)
    ]
    columns = jnp.concatenate([total.astype(jnp.bfloat16) for total in sums], axis=1)
    grams = [
        jnp.dot(total.T.astype(jnp.bfloat16), columns, preferred_element_type=jnp.float32).astype(jnp.bfloat16)
        for total in sums
    ]
    block = out_ref.shape[1]
    for i, (col, row) in enumerate(targets):
        out_ref[i] = grams[row][col * block : (col + 1) * block]


def partial_gram(met, rows_of, targets, parts, rows, halves):
    return pl.pallas_call(
        functools.partial(gram_kernel, rows_of=rows_of, targets=targets, halves=halves),
        out_shape=pltpu.VMEM((len(targets), rows // parts, halves * rows), jnp.bfloat16),
        in_specs=[pl.BlockSpec(memory_space=pltpu.VMEM)],
        out_specs=pl.BlockSpec(memory_space=pltpu.VMEM),
        compiler_params=pltpu.CompilerParams(vmem_limit_bytes=16 << 20),
        name="partial_gram",
    )(met)


def exchange(blocks, axes, order):
    return lax.all_to_all(blocks, axes, split_axis=0, concat_axis=0, tiled=True, axis_index_groups=[order])


def by_pair(part, parts, halves):
    rows = part.shape[1]
    size = parts * halves
    leader = (parts // 2 + 2) * halves - 1
    first = [leader ^ i for i in range(size)]
    second = [(leader + 5 * i) % size for i in range(size)]
    met = exchange(part.reshape(size, -1, rows), ("col", "row"), first)
    rows_of = [i % halves for i in first]
    targets = [(i // halves, i % halves) for i in second]
    return exchange(partial_gram(met, rows_of, targets, parts, rows, halves), ("col", "row"), second)


def by_column(part, parts, halves):
    rows = part.shape[1]
    order = [(parts // 2 + 1 + 3 * i) % parts for i in range(parts)]
    met = exchange(part.reshape(parts, -1, rows), "col", order)
    sketch = (met.astype(jnp.float32).sum(0) / SIDE).astype(jnp.bfloat16)
    both = lax.all_gather(sketch, "row", axis=1, tiled=True)
    gram = lax.dot_general(sketch, both, (((0,), (0,)), ((), ())), preferred_element_type=jnp.float32)
    blocks = gram.astype(jnp.bfloat16).reshape(parts, rows // parts, -1)
    return exchange(jnp.concatenate([blocks[i : i + 1] for i in order]), "col", order)


def per_device(parts, halves, theta, signs, kept):
    keep = kept.shape[0]
    part = partial_sketch(theta, signs, kept)
    whole_tiles = keep % (parts * halves * TILE) == 0
    met = (by_pair if whole_tiles else by_column)(part, parts, halves)
    return (met.astype(jnp.float32).sum(0) / keep)[None, None]


def solution(mesh):
    return jax.shard_map(
        functools.partial(per_device, mesh.shape["col"], mesh.shape["row"]),
        mesh=mesh,
        in_specs=(P(("real", "row"), "col"), P(("real", "col")), P()),
        out_specs=P(("real", "row"), "col", None, None),
        check_vma=False,
    )
```

```python
import functools

import jax
import jax.numpy as jnp
from jax import lax
from jax.experimental import pallas as pl
from jax.experimental.pallas import tpu as pltpu
from jax.sharding import PartitionSpec as P

SIDE = 128
STRIPS = 4
TILE = 16


def sign_of(bits, shift=4):
    while shift:
        bits = bits ^ bits >> shift
        shift //= 2
    return (1 - 2 * (bits & 1)).astype(jnp.float32).astype(jnp.bfloat16)


def partial_kernel(theta_hbm, signs_hbm, kept_hbm, out_ref, theta_ref, signs_ref, kept_ref, table_ref, sems):
    copies = [
        pltpu.make_async_copy(source, target, sems.at[i])
        for i, (source, target) in enumerate(((theta_hbm, theta_ref), (kept_hbm, kept_ref), (signs_hbm, signs_ref)))
    ]
    for copy in copies:
        copy.start()
    local = theta_ref.shape[1]
    keep = kept_ref.shape[1]
    groups = local // SIDE
    first = lax.axis_index("col") * groups
    strip = keep // STRIPS

    def sign_rows(count, bits):
        return sign_of(lax.broadcasted_iota(jnp.int32, (count, strip), 0) & bits)

    def build(s):
        kept = kept_ref[:, s * strip : (s + 1) * strip]
        low, middle = sign_rows(TILE, kept & (TILE - 1)), sign_rows(SIDE // TILE, kept // TILE & (SIDE // TILE - 1))
        inner = jnp.concatenate([low * middle[i : i + 1] for i in range(SIDE // TILE)], axis=0)
        high = sign_of((first + lax.broadcasted_iota(jnp.int32, (groups, strip), 0)) & (kept >> 7))
        for group in range(groups):
            table_ref[group * SIDE : (group + 1) * SIDE, s * strip : (s + 1) * strip] = inner * high[group : group + 1]

    copies[1].wait()
    build(0)
    build(1)
    copies[2].wait()
    copies[0].wait()
    theta_ref[...] = theta_ref[...] * signs_ref[...].astype(jnp.float32).astype(jnp.bfloat16)
    for s in range(STRIPS):
        if s + 2 < STRIPS:
            build(s + 2)
        part = jnp.dot(theta_ref[...], table_ref[:, s * strip : (s + 1) * strip], preferred_element_type=jnp.float32)
        out_ref[s * strip : (s + 1) * strip, :] = part.T.astype(jnp.bfloat16)


def partial_sketch(theta, signs, kept):
    rows, local = theta.shape
    keep = kept.shape[0]
    inputs = (theta, signs.reshape(1, local), kept.reshape(1, keep))
    return pl.pallas_call(
        partial_kernel,
        out_shape=pltpu.VMEM((keep, rows), jnp.bfloat16),
        in_specs=[pl.BlockSpec(memory_space=pltpu.HBM)] * 3,
        out_specs=pl.BlockSpec(memory_space=pltpu.VMEM),
        scratch_shapes=[
            pltpu.VMEM((rows, local), jnp.bfloat16),
            pltpu.VMEM((1, local), jnp.int32),
            pltpu.VMEM((1, keep), jnp.int32),
            pltpu.VMEM((local, keep), jnp.bfloat16),
            pltpu.SemaphoreType.DMA((3,)),
        ],
        compiler_params=pltpu.CompilerParams(vmem_limit_bytes=32 << 20),
        name="partial_sketch",
    )(*(pltpu.with_memory_space_constraint(x, pltpu.HBM) for x in inputs))


def gram_kernel(met_ref, out_ref, *, rows_of, targets, halves):
    sums = [
        sum(met_ref[i].astype(jnp.float32) for i, row in enumerate(rows_of) if row == half) * (1 / SIDE)
        for half in range(halves)
    ]
    columns = jnp.concatenate([total.astype(jnp.bfloat16) for total in sums], axis=1)
    grams = [
        jnp.dot(total.T.astype(jnp.bfloat16), columns, preferred_element_type=jnp.float32).astype(jnp.bfloat16)
        for total in sums
    ]
    block = out_ref.shape[1]
    for i, (col, row) in enumerate(targets):
        out_ref[i] = grams[row][col * block : (col + 1) * block]


def partial_gram(met, rows_of, targets, parts, rows, halves):
    return pl.pallas_call(
        functools.partial(gram_kernel, rows_of=rows_of, targets=targets, halves=halves),
        out_shape=pltpu.VMEM((len(targets), rows // parts, halves * rows), jnp.bfloat16),
        in_specs=[pl.BlockSpec(memory_space=pltpu.VMEM)],
        out_specs=pl.BlockSpec(memory_space=pltpu.VMEM),
        compiler_params=pltpu.CompilerParams(vmem_limit_bytes=16 << 20),
        name="partial_gram",
    )(met)


def exchange(blocks, axes, order):
    return lax.all_to_all(blocks, axes, split_axis=0, concat_axis=0, tiled=True, axis_index_groups=[order])


def member_order(size, leader, step, runs):
    cut = size // runs
    return [(leader + step * (i % cut * runs + i // cut)) % size for i in range(size)]


def by_pair(part, parts, halves):
    rows = part.shape[1]
    size = parts * halves
    leader = (parts // 2 + 2) * halves - 1
    first, second = member_order(size, leader, 7, 4), member_order(size, leader, 9, 8)
    met = exchange(part.reshape(size, -1, rows), ("col", "row"), first)
    rows_of = [i % halves for i in first]
    targets = [(i // halves, i % halves) for i in second]
    return exchange(partial_gram(met, rows_of, targets, parts, rows, halves), ("col", "row"), second)


def by_column(part, parts, halves):
    rows = part.shape[1]
    order = [(parts // 2 + 1 + 3 * i) % parts for i in range(parts)]
    met = exchange(part.reshape(parts, -1, rows), "col", order)
    sketch = (met.astype(jnp.float32).sum(0) / SIDE).astype(jnp.bfloat16)
    both = lax.all_gather(sketch, "row", axis=1, tiled=True)
    gram = lax.dot_general(sketch, both, (((0,), (0,)), ((), ())), preferred_element_type=jnp.float32)
    blocks = gram.astype(jnp.bfloat16).reshape(parts, rows // parts, -1)
    return exchange(jnp.concatenate([blocks[i : i + 1] for i in order]), "col", order)


def per_device(parts, halves, theta, signs, kept):
    keep = kept.shape[0]
    part = partial_sketch(theta, signs, kept)
    whole_tiles = keep % (parts * halves * TILE) == 0
    met = (by_pair if whole_tiles else by_column)(part, parts, halves)
    return (met.astype(jnp.float32).sum(0) / keep)[None, None]


def solution(mesh):
    return jax.shard_map(
        functools.partial(per_device, mesh.shape["col"], mesh.shape["row"]),
        mesh=mesh,
        in_specs=(P(("real", "row"), "col"), P(("real", "col")), P()),
        out_specs=P(("real", "row"), "col", None, None),
        check_vma=False,
    )
```

```python
import functools

import jax
import jax.numpy as jnp
from jax import lax
from jax.experimental import pallas as pl
from jax.experimental.pallas import tpu as pltpu
from jax.sharding import PartitionSpec as P

SIDE = 128
STRIPS = 4
TILE = 16


def sign_of(bits, shift=4):
    while shift:
        bits = bits ^ bits >> shift
        shift //= 2
    return (1 - 2 * (bits & 1)).astype(jnp.float32).astype(jnp.bfloat16)


def partial_kernel(theta_hbm, signs_hbm, kept_hbm, out_ref, theta_ref, signs_ref, kept_ref, table_ref, sems):
    copies = [
        pltpu.make_async_copy(source, target, sems.at[i])
        for i, (source, target) in enumerate(((theta_hbm, theta_ref), (kept_hbm, kept_ref), (signs_hbm, signs_ref)))
    ]
    for copy in copies:
        copy.start()
    local = theta_ref.shape[1]
    keep = kept_ref.shape[1]
    groups = local // SIDE
    first = lax.axis_index("col") * groups
    strip = keep // STRIPS

    def sign_rows(count, bits):
        return sign_of(lax.broadcasted_iota(jnp.int32, (count, strip), 0) & bits)

    def build(s):
        kept = kept_ref[:, s * strip : (s + 1) * strip]
        low, middle = sign_rows(TILE, kept & (TILE - 1)), sign_rows(SIDE // TILE, kept // TILE & (SIDE // TILE - 1))
        inner = jnp.concatenate([low * middle[i : i + 1] for i in range(SIDE // TILE)], axis=0)
        high = sign_of((first + lax.broadcasted_iota(jnp.int32, (groups, strip), 0)) & (kept >> 7))
        for group in range(groups):
            table_ref[group * SIDE : (group + 1) * SIDE, s * strip : (s + 1) * strip] = inner * high[group : group + 1]

    copies[1].wait()
    build(0)
    build(1)
    copies[2].wait()
    copies[0].wait()
    theta_ref[...] = theta_ref[...] * signs_ref[...].astype(jnp.float32).astype(jnp.bfloat16)
    for s in range(STRIPS):
        if s + 2 < STRIPS:
            build(s + 2)
        part = jnp.dot(theta_ref[...], table_ref[:, s * strip : (s + 1) * strip], preferred_element_type=jnp.float32)
        out_ref[s * strip : (s + 1) * strip, :] = part.T.astype(jnp.bfloat16)


def partial_sketch(theta, signs, kept):
    rows, local = theta.shape
    keep = kept.shape[0]
    inputs = (theta, signs.reshape(1, local), kept.reshape(1, keep))
    return pl.pallas_call(
        partial_kernel,
        out_shape=pltpu.VMEM((keep, rows), jnp.bfloat16),
        in_specs=[pl.BlockSpec(memory_space=pltpu.HBM)] * 3,
        out_specs=pl.BlockSpec(memory_space=pltpu.VMEM),
        scratch_shapes=[
            pltpu.VMEM((rows, local), jnp.bfloat16),
            pltpu.VMEM((1, local), jnp.int32),
            pltpu.VMEM((1, keep), jnp.int32),
            pltpu.VMEM((local, keep), jnp.bfloat16),
            pltpu.SemaphoreType.DMA((3,)),
        ],
        compiler_params=pltpu.CompilerParams(vmem_limit_bytes=32 << 20),
        name="partial_sketch",
    )(*(pltpu.with_memory_space_constraint(x, pltpu.HBM) for x in inputs))


def gram_kernel(met_ref, out_ref, *, rows_of, targets, halves):
    sums = [
        sum(met_ref[i].astype(jnp.float32) for i, row in enumerate(rows_of) if row == half) * (1 / SIDE)
        for half in range(halves)
    ]
    columns = jnp.concatenate([total.astype(jnp.bfloat16) for total in sums], axis=1)
    contract = (((0,), (0,)), ((), ()))
    gram = lax.dot_general(columns, columns, contract, preferred_element_type=jnp.float32).astype(jnp.bfloat16)
    rows = gram.shape[0] // halves
    block = out_ref.shape[1]
    for i, (col, row) in enumerate(targets):
        start = row * rows + col * block
        out_ref[i] = gram[start : start + block]


def partial_gram(met, rows_of, targets, parts, rows, halves):
    return pl.pallas_call(
        functools.partial(gram_kernel, rows_of=rows_of, targets=targets, halves=halves),
        out_shape=pltpu.VMEM((len(targets), rows // parts, halves * rows), jnp.bfloat16),
        in_specs=[pl.BlockSpec(memory_space=pltpu.VMEM)],
        out_specs=pl.BlockSpec(memory_space=pltpu.VMEM),
        compiler_params=pltpu.CompilerParams(vmem_limit_bytes=16 << 20),
        name="partial_gram",
    )(met)


def exchange(blocks, axes, order):
    return lax.all_to_all(blocks, axes, split_axis=0, concat_axis=0, tiled=True, axis_index_groups=[order])


def member_order(size, leader, step, runs):
    cut = size // runs
    return [(leader + step * (i % cut * runs + i // cut)) % size for i in range(size)]


def by_pair(part, parts, halves):
    rows = part.shape[1]
    size = parts * halves
    leader = (parts // 2 + 2) * halves - 1
    first, second = member_order(size, leader, 7, 4), member_order(size, leader, 9, 8)
    met = exchange(part.reshape(size, -1, rows), ("col", "row"), first)
    rows_of = [i % halves for i in first]
    targets = [(i // halves, i % halves) for i in second]
    return exchange(partial_gram(met, rows_of, targets, parts, rows, halves), ("col", "row"), second)


def by_column(part, parts, halves):
    rows = part.shape[1]
    order = [(parts // 2 + 1 + 3 * i) % parts for i in range(parts)]
    met = exchange(part.reshape(parts, -1, rows), "col", order)
    sketch = (met.astype(jnp.float32).sum(0) / SIDE).astype(jnp.bfloat16)
    both = lax.all_gather(sketch, "row", axis=1, tiled=True)
    gram = lax.dot_general(sketch, both, (((0,), (0,)), ((), ())), preferred_element_type=jnp.float32)
    blocks = gram.astype(jnp.bfloat16).reshape(parts, rows // parts, -1)
    return exchange(jnp.concatenate([blocks[i : i + 1] for i in order]), "col", order)


def per_device(parts, halves, theta, signs, kept):
    keep = kept.shape[0]
    part = partial_sketch(theta, signs, kept)
    whole_tiles = keep % (parts * halves * TILE) == 0
    met = (by_pair if whole_tiles else by_column)(part, parts, halves)
    return (met.astype(jnp.float32).sum(0) / keep)[None, None]


def solution(mesh):
    return jax.shard_map(
        functools.partial(per_device, mesh.shape["col"], mesh.shape["row"]),
        mesh=mesh,
        in_specs=(P(("real", "row"), "col"), P(("real", "col")), P()),
        out_specs=P(("real", "row"), "col", None, None),
        check_vma=False,
    )
```
